32 devices in a mesh: parts: 2 (over y), blk: 4 (over z), dp: 2 (over x), sub: 2 (over core).
Axes of the slice: x: 2, y: 2, z: 4, core: 2. Of those that a mesh axis runs over, the one named last changes fastest.
Arguments:
- in_factors: bfloat16 [2, 4, 512, 1024], P(None, ('parts', 'dp'), 'blk'), parts along dimension 1, may hold values from -6 to 6
- out_factors: bfloat16 [2, 4, 512, 1024], P(None, ('parts', 'dp'), 'blk'), parts along dimension 1, may hold values from -0.75 to 0.75
- lengths: int32 [4, 32], P(('parts', 'dp')), parts along dimension 0, may hold values from 1 to 64, 512 in all within a row
- signs: int32 [2, 1024, 1024], P(None, 'blk'), may hold values 0 or 1
- projection: bfloat16 [2, 1024, 16, 4096], P(None, 'blk', None, 'sub'), may hold values from -0.046875 to 0.046875
Outputs:
- features: float32 [4, 32, 2, 4096], P(('parts', 'dp'), 'blk', None, 'sub'), parts along dimension 0
The draws below stay inside these ranges and needn't reach their ends.
There are 2 independent parts, one for each index of `parts`. The reference program is written for one: setup_inputs(seed, part) draws one part's arguments, and reference() takes and returns one part's arrays. A program takes and returns all parts, laid end to end along the dimension named above; an argument that names none is the same for every part. Nothing has to cross between parts.
Inputs may be any that keep to these rules, and one draw needn't show every extreme that they name: In each row the 32 lengths sum to 512; the documents follow one another over the tokens of their dp index in order.
All inputs are finite; a program needn't handle non-finite values. No bound on the sum of `signs` on one device may be relied on, other than what follows from the above.
Results may differ from the reference program's by a relative error of at most 0.0029.
Values may be sent and summed in bfloat16 or wider, within the bound.
No kernel may reach another device: no remote copies, remote signals or barrier semaphores. Data moves between devices by JAX's collectives and lax.ppermute only.
A program may use at most 128 MiB of HBM per device.

```python
import math
import jax
import jax.numpy as jnp
import numpy as np
from jax import lax

IN_DIM = 1024
OUT_DIM = 1024
PROJ = 4096
KEEP = 16
LAYERS = 2
EX_DEV = 32
TOK_DEV = 512
LEN_MAX = 64
N_DP = 2


def touch_ends(result, stream_key, smallest, largest):
    shape = result.shape
    spot = [jax.random.randint(jax.random.fold_in(stream_key, axis), (), 0, shape[axis]) for axis in range(len(shape))]
    result = result.at[tuple(spot)].set(smallest)
    longest = shape.index(max(shape))
    spot[longest] = (spot[longest] + 1) % shape[longest]
    return result.at[tuple(spot)].set(largest)


def level_of(rng, shape, cuts, least, high):
    gain, own = 1.0, jax.random.fold_in(rng, 6)
    for position, blocks in cuts:
        draws = jnp.exp(jax.random.uniform(jax.random.fold_in(own, position), (blocks,), jnp.float32, least / len(cuts), high / len(cuts)))
        gain = gain * jnp.repeat(draws, shape[position] // blocks).reshape([-1 if axis == position else 1 for axis in range(len(shape))])
    return gain


def split_up(count, total, most, skew):
    portions = [(1 << 20) // math.isqrt(grade ** skew) + 1 for grade in range(2, count + 1)]
    spare, holding = total - most - (count - 1), [1] * (count - 1)
    while spare > 0:
        free = [i for i in range(count - 1) if holding[i] < most]
        mass, remaining = sum([portions[i] for i in free]), spare
        for i in free:
            more = min(most - holding[i], max(1, remaining * portions[i] // mass), spare)
            holding[i] = holding[i] + more
            spare = spare - more
    return np.array([most] + holding)


def uneven(key, number_of, total, reach, slope):
    if number_of == 2:
        one = jax.random.randint(key, (), max(1, total - reach), min(reach, total - 1) + 1)
        return jnp.stack([one, total - one])
    tallies = jnp.asarray(split_up(number_of, total, reach, slope), jnp.int32)
    twos = (number_of - 1) // 2
    source_of, receiver = tallies[1:1 + 2 * twos:2], tallies[2:2 + 2 * twos:2]
    slack = jnp.minimum(source_of - 1, reach - receiver)
    moved = jax.random.randint(jax.random.fold_in(key, 1), (twos,), 0, 1 << 20) % (slack + 1)
    tallies = tallies.at[1:1 + 2 * twos:2].set(source_of - moved).at[2:2 + 2 * twos:2].set(receiver + moved)
    return tallies[jax.random.permutation(jax.random.fold_in(key, 2), number_of)]


def normal_values(key, shape, width, bound, pieces=(), kind=jnp.bfloat16):
    array = jax.random.normal(key, shape, jnp.float32) * width
    if len(pieces) > 0:
        array = level_of(key, shape, pieces, -0.22, 0.18) * array
    return jnp.clip(array, min=-bound, max=bound).astype(kind)


def setup_inputs(seed: int = 0, part: int = 0) -> dict:
    keys = jax.random.split(jax.random.key(seed), 6)
    part_splits = jax.random.split(jax.random.fold_in(keys[5], part), 6)
    return {
        "in_factors": normal_values(part_splits[0], (LAYERS, N_DP, TOK_DEV, IN_DIM), 1.0, 6.0, ((1, 2), (2, 4))),
        "out_factors": normal_values(part_splits[1], (LAYERS, N_DP, TOK_DEV, OUT_DIM), 0.125, 0.75, ((1, 2), (2, 4))),
        "lengths": jax.vmap(lambda own: uneven(own, EX_DEV, TOK_DEV, LEN_MAX, 2))(jax.random.split(part_splits[2], N_DP)).reshape((N_DP, EX_DEV)).astype(jnp.int32),
        "signs": touch_ends((jax.random.randint(keys[3], (LAYERS, IN_DIM, OUT_DIM), 0, 2) < 1).astype(jnp.int32), jax.random.fold_in(keys[3], 1), 0, 1),
        "projection": normal_values(keys[4], (LAYERS, IN_DIM, KEEP, PROJ), (IN_DIM * KEEP) ** -0.5, 0.046875, ((1, 4), (3, 2))),
    }


def parity_sign(values):
    total = jnp.zeros_like(values)
    for bit_level in range(16):
        total = total + jnp.bitwise_and(jnp.right_shift(values, bit_level), 1)
    return (1 - 2 * (total % 2)).astype(jnp.float32)

def parity_table(row_ids, col_ids):
    return parity_sign(jnp.bitwise_and(row_ids[:, None], col_ids[None, :]))

def reference(in_factors, out_factors, lengths, signs, projection):
    norm_scale = 1.0 / math.sqrt(IN_DIM * OUT_DIM)
    row_ids = jnp.arange(IN_DIM, dtype=jnp.int32)
    col_ids = jnp.arange(OUT_DIM, dtype=jnp.int32)
    kept_ids = jnp.arange(KEEP, dtype=jnp.int32)
    row_mix = parity_table(row_ids, row_ids)
    col_mix = parity_table(col_ids, kept_ids)
    window_ids = jnp.arange(LEN_MAX, dtype=jnp.int32)
    shards = []
    for dp_shard in range(N_DP):
        doc_lengths = lengths[dp_shard].astype(jnp.int32)
        doc_starts = (jnp.cumsum(doc_lengths) - doc_lengths).astype(jnp.int32)
        per_layer = []
        for layer_id in range(LAYERS):
            signed = (2 * signs[layer_id] - 1).astype(jnp.float32)
            mixing = signed[:, :, None] * col_mix[None, :, :]
            left_pad = jnp.pad(in_factors[layer_id, dp_shard].astype(jnp.float32), ((0, LEN_MAX), (0, 0)))
            right_pad = jnp.pad(out_factors[layer_id, dp_shard].astype(jnp.float32), ((0, LEN_MAX), (0, 0)))

            def one_example(bounds):
                offset, length = bounds
                left_window = lax.dynamic_slice_in_dim(left_pad, offset, LEN_MAX, 0)
                right_window = lax.dynamic_slice_in_dim(right_pad, offset, LEN_MAX, 0)
                inside = (window_ids < length)[:, None]
                left_window = jnp.where(inside, left_window, jnp.zeros_like(left_window))
                gradient = jnp.dot(left_window.T, right_window, precision=lax.Precision.HIGHEST)
                return jnp.einsum('ic,ick->ik', gradient, mixing, precision=lax.Precision.HIGHEST)
            folded = lax.map(one_example, (doc_starts, doc_lengths))
            transformed = jnp.einsum('ji,eik->ejk', row_mix, folded, precision=lax.Precision.HIGHEST) * norm_scale
            kept = transformed.astype(jnp.bfloat16).reshape(EX_DEV, IN_DIM * KEEP)
            weights = projection[layer_id].reshape(IN_DIM * KEEP, PROJ)
            per_layer.append(jnp.dot(kept, weights, preferred_element_type=jnp.float32))
        shards.append(jnp.stack(per_layer, axis=1))
    return jnp.stack(shards, axis=0)
```

```python
import functools
import math

import jax
import jax.numpy as jnp
from jax import lax
from jax.experimental import pallas as pl
from jax.experimental.pallas import tpu as pltpu
from jax.sharding import PartitionSpec as P

F32 = jnp.float32
BF16 = jnp.bfloat16
NT = (((1,), (1,)), ((), ()))


def parity_sign(values):
    for shift in (8, 4, 2, 1):
        values = jnp.bitwise_xor(values, jnp.right_shift(values, shift))
    return (1 - 2 * jnp.bitwise_and(values, 1)).astype(F32)


def iota(shape, dim):
    return lax.broadcasted_iota(jnp.int32, shape, dim)


def split_bf16(x):
    hi = x.astype(BF16)
    return hi, (x - hi.astype(F32)).astype(BF16)


def fold_kernel(blocks, kept, ids_ref, lengths_ref, signs_ref, left_ref, *refs):
    own_ref = refs[0]
    up_refs = refs[1:blocks]
    down_refs = refs[blocks:2 * blocks - 1]
    out_ref, b_scr, a_scr, h_scr, hot_scr = refs[2 * blocks - 1:]
    tokens, width = b_scr.shape
    tok_local = tokens // blocks
    documents = hot_scr.shape[0]
    me = ids_ref[1]

    @pl.when(pl.program_id(0) == 0)
    def _():
        def place(ref, block):
            b_scr[pl.ds(pl.multiple_of(block * tok_local, tok_local), tok_local), :] = ref[...]

        place(own_ref, me)
        for step in range(1, blocks):
            pl.when(me - step >= 0)(functools.partial(place, up_refs[step - 1], me - step))
            pl.when(me + step < blocks)(functools.partial(place, down_refs[step - 1], me + step))
        for block in range(blocks):
            a_scr[:, block * tok_local:(block + 1) * tok_local] = left_ref[block].astype(F32)
        h_scr[...] = parity_sign(jnp.bitwise_and(iota(h_scr.shape, 0), iota(h_scr.shape, 1)))
        square = (documents, documents)
        spread = jnp.broadcast_to(lengths_ref[...].astype(F32), square)
        ends = jnp.sum(jnp.where(iota(square, 1) <= iota(square, 0), spread, 0.0), axis=1, keepdims=True)
        starts = jnp.sum(jnp.where(iota(square, 1) < iota(square, 0), spread, 0.0), axis=1, keepdims=True)
        token = iota((documents, tokens), 1).astype(F32)
        hot = jnp.where((token >= starts) & (token < ends), 1.0, 0.0).astype(BF16)
        hot_scr[:, :tokens] = hot
        hot_scr[:, tokens:] = hot

    rows = signs_ref.shape[1]
    row0 = pl.multiple_of(pl.program_id(0) * rows, rows)
    signed = (2 * signs_ref[0] - 1).astype(F32)
    mixing = (signed[:, None, :] * h_scr[...][None]).reshape(rows * kept, width).astype(BF16)
    mixed = lax.dot_general(mixing, b_scr[...], NT, preferred_element_type=F32)
    left = a_scr[pl.ds(row0, rows), :]
    terms = (mixed.reshape(rows, kept, tokens) * left[:, None, :]).reshape(rows * kept, tokens)
    hi, lo = split_bf16(terms)
    out_ref[...] = lax.dot_general(
        hot_scr[...], jnp.concatenate([hi, lo], axis=1), NT, preferred_element_type=F32
    )


def fold(ids, lengths, signs, left, own, up, down, kept):
    blocks, rows_block, tok_local = left.shape
    width = own.shape[1]
    tokens = blocks * tok_local
    documents = lengths.shape[1]
    rows = min(16, rows_block)
    whole = lambda shape: pl.BlockSpec(shape, lambda g, ids: (0,) * len(shape))
    return pl.pallas_call(
        functools.partial(fold_kernel, blocks, kept),
        grid_spec=pltpu.PrefetchScalarGridSpec(
            num_scalar_prefetch=1,
            grid=(rows_block // rows,),
            in_specs=[
                whole(lengths.shape),
                pl.BlockSpec((1, rows, width), lambda g, ids: (ids[0], g, 0)),
                whole(left.shape),
            ] + [whole(own.shape)] * (2 * blocks - 1),
            out_specs=pl.BlockSpec((documents, rows * kept), lambda g, ids: (0, g)),
            scratch_shapes=[
                pltpu.VMEM((tokens, width), BF16),
                pltpu.VMEM((rows_block, tokens), F32),
                pltpu.VMEM((kept, width), F32),
                pltpu.VMEM((documents, 2 * tokens), BF16),
            ],
        ),
        out_shape=jax.ShapeDtypeStruct((documents, rows_block * kept), F32),
        name="fold",
    )(ids, lengths, signs, left, own, *up, *down)


def mix_kernel(blocks, kept, scale, in_ref, out_ref):
    rows, lanes = in_ref.shape
    docs = rows // blocks
    tile = min(256, lanes)
    count = lanes // tile
    row, col = iota((tile, tile), 0), iota((tile, tile), 1)
    same = jnp.bitwise_and(row, kept - 1) == jnp.bitwise_and(col, kept - 1)
    table = parity_sign(jnp.bitwise_and(row // kept, col // kept))
    table = jnp.where(same, table, 0.0).astype(BF16)
    stacked = jnp.concatenate([in_ref[:, t * tile:(t + 1) * tile] for t in range(count)], axis=0)
    hi, lo = split_bf16(stacked)
    both = jnp.dot(jnp.concatenate([hi, lo], axis=0), table, preferred_element_type=F32)
    both = both[:count * rows] + both[count * rows:]
    parts = [[both[t * rows + b * docs:t * rows + (b + 1) * docs] for b in range(blocks)] for t in range(count)]

    def butterfly(items):
        step = 1
        while step < len(items):
            for low in range(len(items)):
                if not low & step:
                    a, b = items[low], items[low | step]
                    items[low], items[low | step] = a + b, a - b
            step *= 2
        return items

    for b in range(blocks):
        column = butterfly([parts[t][b] for t in range(count)])
        for t in range(count):
            parts[t][b] = column[t]
    for t in range(count):
        done = butterfly(parts[t])
        for b in range(blocks):
            out_ref[b * docs:(b + 1) * docs, t * tile:(t + 1) * tile] = (done[b] * scale).astype(BF16)


def mix(folded, blocks, kept, scale):
    return pl.pallas_call(
        functools.partial(mix_kernel, blocks, kept, scale),
        out_shape=jax.ShapeDtypeStruct(folded.shape, BF16),
        name="mix",
    )(folded)


def project_kernel(ids_ref, kept_ref, weights_ref, out_ref, acc_ref):
    step = pl.program_id(0)

    @pl.when(step == 0)
    def _():
        acc_ref[...] = jnp.zeros_like(acc_ref)

    acc_ref[...] += jnp.dot(kept_ref[...], weights_ref[0], preferred_element_type=F32)

    @pl.when(step == pl.num_programs(0) - 1)
    def _():
        out_ref[...] = acc_ref[...].astype(out_ref.dtype)


def project(layer, kept, weights):
    documents, depth = kept.shape
    width = weights.shape[2]
    part = min(512, depth)
    return pl.pallas_call(
        project_kernel,
        grid_spec=pltpu.PrefetchScalarGridSpec(
            num_scalar_prefetch=1,
            grid=(depth // part,),
            in_specs=[
                pl.BlockSpec((documents, part), lambda g, ids: (0, g)),
                pl.BlockSpec((1, part, width), lambda g, ids: (ids[0], g, 0)),
            ],
            out_specs=pl.BlockSpec((documents, width), lambda g, ids: (0, 0)),
            scratch_shapes=[pltpu.VMEM((documents, width), F32)],
        ),
        out_shape=jax.ShapeDtypeStruct((documents, width), BF16),
        name="project",
        cost_estimate=pl.CostEstimate(
            flops=2 * documents * depth * width, bytes_accessed=2 * depth * width, transcendentals=0
        ),
    )(layer, kept, weights)


def line(block, count, step):
    return lax.ppermute(block, "blk", [(i, i + step) for i in range(count) if 0 <= i + step < count])


def exchange(rows):
    return lax.all_to_all(rows, "blk", split_axis=0, concat_axis=0, tiled=True)


def shards(in_factors, out_factors, lengths, signs, projection):
    blocks = lax.axis_size("blk")
    halves = lax.axis_size("sub")
    my_block = lax.axis_index("blk")
    my_half = lax.axis_index("sub")
    layers, _, tok_local, in_width = in_factors.shape
    out_width = out_factors.shape[3]
    assert layers == halves == 2
    rows_block = in_width // blocks
    documents = lengths.shape[1]
    docs = documents // blocks
    kept_cols = projection.shape[2]
    scale = 1.0 / math.sqrt(in_width * out_width)

    own = lax.dynamic_index_in_dim(out_factors[:, 0], my_half, 0, keepdims=False)
    left = lax.dynamic_index_in_dim(in_factors[:, 0], my_half, 0, keepdims=False)
    left = exchange(left.T.reshape(blocks, rows_block, tok_local))
    up, down = [], []
    for step in range(1, blocks):
        up.append(line(up[-1] if up else own, blocks, 1))
        down.append(line(down[-1] if down else own, blocks, -1))
    ids = jnp.stack([my_half, my_block]).astype(jnp.int32)
    folded = fold(ids, lengths, signs, left, own, up, down, kept_cols)
    folded = exchange(folded)
    kept = exchange(mix(folded, blocks, kept_cols, scale))
    other = lax.ppermute(kept, "sub", [(0, 1), (1, 0)])
    weights = projection.reshape(layers, rows_block * kept_cols, projection.shape[3])
    width = weights.shape[2]
    mine = project(ids[:1], kept, weights)
    theirs = project(1 - ids[:1], other, weights)
    mine = exchange(mine).reshape(blocks, docs, width).astype(F32)
    theirs = exchange(theirs).reshape(blocks, docs, width).astype(F32)
    mine, theirs = jnp.sum(mine, axis=0), jnp.sum(theirs, axis=0)
    first = my_half == 0
    return jnp.stack([jnp.where(first, mine, theirs), jnp.where(first, theirs, mine)], axis=1)[None]


def solution(mesh):
    return jax.shard_map(
        shards,
        mesh=mesh,
        in_specs=(
            P(None, ("parts", "dp"), "blk", None),
            P(None, ("parts", "dp"), "blk", None),
            P(("parts", "dp"), None),
            P(None, "blk", None),
            P(None, "blk", None, "sub"),
        ),
        out_specs=P(("parts", "dp"), "blk", None, "sub"),
        check_vma=False,
    )
```

```python
import functools
import math

import jax
import jax.numpy as jnp
from jax import lax
from jax.experimental import pallas as pl
from jax.experimental.pallas import tpu as pltpu
from jax.sharding import PartitionSpec as P


F32 = jnp.float32
BF16 = jnp.bfloat16
NT = (((1,), (1,)), ((), ()))
FINE = 4
SMEM_SPEC = pl.BlockSpec(memory_space=pltpu.SMEM)
VMEM_SPEC = pl.BlockSpec(memory_space=pltpu.VMEM)
HBM_SPEC = pl.BlockSpec(memory_space=pltpu.HBM)


def params(mib):
    return pltpu.CompilerParams(vmem_limit_bytes=mib << 20)


def iota(shape, dim):
    return lax.broadcasted_iota(jnp.int32, shape, dim)


def parity_sign(values):
    for shift in (8, 4, 2, 1):
        values = jnp.bitwise_xor(values, jnp.right_shift(values, shift))
    return (1 - 2 * jnp.bitwise_and(values, 1)).astype(F32)


def split_bf16(x):
    hi = x.astype(BF16)
    return hi, (x - hi.astype(F32)).astype(BF16)


def prepare_kernel(kept, ids_ref, signs_ref, spread_ref, order_ref):
    _, width = signs_ref.shape[1:]
    coarse = kept // FINE
    part = width // coarse
    source = iota((width, width), 0)
    place = (source // FINE) % coarse * part + source // kept * FINE + source % FINE
    order_ref[...] = jnp.where(place == iota((width, width), 1), 1.0, 0.0).astype(BF16)
    signed = (2 * signs_ref[ids_ref[0]] - 1).astype(F32).astype(BF16)
    for c in range(coarse):
        cols = slice(c * part, (c + 1) * part)
        piece = jnp.dot(signed, order_ref[:, cols], preferred_element_type=F32)
        for f in range(FINE):
            spread_ref[c, f] = jnp.where(iota(piece.shape, 1) % FINE == f, piece, 0.0).astype(BF16)


def prepare(ids, signs, kept):
    rows, width = signs.shape[1:]
    coarse = kept // FINE
    return pl.pallas_call(
        functools.partial(prepare_kernel, kept),
        in_specs=[SMEM_SPEC, VMEM_SPEC],
        out_specs=[VMEM_SPEC, VMEM_SPEC],
        out_shape=[
            jax.ShapeDtypeStruct((coarse, FINE, rows, width // coarse), BF16),
            jax.ShapeDtypeStruct((width, width), BF16),
        ],
        name="prepare",
        compiler_params=params(8),
        cost_estimate=pl.CostEstimate(flops=16_000_000, bytes_accessed=8 * rows * width, transcendentals=0),
    )(ids, signs)


def fetch_kernel(pick, ids_ref, weights_ref, out_ref, sems):
    layer = ids_ref[0] if pick == 0 else 1 - ids_ref[0]
    count = sems.shape[0]
    part = out_ref.shape[0] // count
    copies = [
        pltpu.make_async_copy(
            weights_ref.at[layer, pl.ds(i * part, part)], out_ref.at[pl.ds(i * part, part)], sems.at[i]
        )
        for i in range(count)
    ]
    for copy in copies:
        copy.start()
    for copy in copies:
        copy.wait()


def fetch(ids, weights, pick):
    depth, width = weights.shape[1:]
    return pl.pallas_call(
        functools.partial(fetch_kernel, pick),
        in_specs=[SMEM_SPEC, HBM_SPEC],
        out_specs=VMEM_SPEC,
        out_shape=jax.ShapeDtypeStruct((depth, width), BF16),
        scratch_shapes=[pltpu.SemaphoreType.DMA((4,))],
        name="fetch",
        compiler_params=params(24 if pick == 0 else 4),
        cost_estimate=pl.CostEstimate(flops=16_000_000, bytes_accessed=2 * depth * width, transcendentals=0),
    )(ids, weights)


def fold_kernel(blocks, kept, tile, ids_ref, lengths_ref, spread_ref, order_ref, left_ref, own_ref, *refs):
    mine_refs, theirs_refs = refs[:blocks - 1], refs[blocks - 1:2 * blocks - 2]
    out_ref, b_scr, a_scr, hot_scr = refs[2 * blocks - 2:]
    tokens, width = b_scr.shape
    tok_local = tokens // blocks
    documents = hot_scr.shape[0]
    coarse = kept // FINE
    part = width // coarse
    half, me = ids_ref[0], ids_ref[1]

    @pl.when(pl.program_id(0) == 0)
    def _():
        def place(value, block):
            rows = pl.ds(pl.multiple_of(block * tok_local, tok_local), tok_local)
            b_scr[rows, :] = jnp.dot(value[...], order_ref[...], preferred_element_type=F32).astype(BF16)

        place(own_ref.at[half], me)
        for step in range(1, blocks):
            toward = jnp.where(half == 0, step, -step)
            for value, block in (
                (mine_refs[step - 1].at[half], me - toward),
                (theirs_refs[step - 1].at[half], me + toward),
            ):
                pl.when((block >= 0) & (block < blocks))(functools.partial(place, value, block))
        for block in range(blocks):
            a_scr[:, block * tok_local:(block + 1) * tok_local] = left_ref[block].astype(F32)
        square = (documents, documents)
        spread = jnp.broadcast_to(lengths_ref[...].astype(F32), square)
        ends = jnp.sum(jnp.where(iota(square, 1) <= iota(square, 0), spread, 0.0), axis=1, keepdims=True)
        starts = jnp.sum(jnp.where(iota(square, 1) < iota(square, 0), spread, 0.0), axis=1, keepdims=True)
        token = iota((documents, tokens), 1).astype(F32)
        hot = jnp.where((token >= starts) & (token < ends), 1.0, 0.0).astype(BF16)
        hot_scr[:, :tokens] = hot
        hot_scr[:, tokens:] = hot

    row0 = pl.multiple_of(pl.program_id(0) * tile, tile)
    left = a_scr[pl.ds(row0, tile), :]
    terms = []
    for c in range(coarse):
        signed = spread_ref[c, :, pl.ds(row0, tile), :].reshape(FINE * tile, part)
        mixed = lax.dot_general(signed, b_scr[:, c * part:(c + 1) * part], NT, preferred_element_type=F32)
        mixed = (mixed.reshape(FINE, tile, tokens) * left[None]).reshape(FINE * tile, tokens)
        terms.append(split_bf16(mixed))
    for u in range(tile // 16):
        pieces = [
            jnp.concatenate(
                [terms[c][w][f * tile + u * 16:f * tile + (u + 1) * 16] for c in range(coarse) for f in range(FINE)],
                axis=0,
            )
            for w in range(2)
        ]
        out_ref[:, u * 16 * kept:(u + 1) * 16 * kept] = lax.dot_general(
            hot_scr[...], jnp.concatenate(pieces, axis=1), NT, preferred_element_type=F32
        )


def fold(ids, lengths, spread, order, left, own, mine, theirs, kept):
    blocks, rows_block, tok_local = left.shape
    width = own.shape[2]
    tokens = blocks * tok_local
    documents = lengths.shape[1]
    tile = min(64, rows_block)
    return pl.pallas_call(
        functools.partial(fold_kernel, blocks, kept, tile),
        grid=(rows_block // tile,),
        in_specs=[SMEM_SPEC] + [VMEM_SPEC] * (5 + 2 * (blocks - 1)),
        out_specs=pl.BlockSpec((documents, tile * kept), lambda g: (0, g)),
        scratch_shapes=[
            pltpu.VMEM((tokens, width), BF16),
            pltpu.VMEM((rows_block, tokens), F32),
            pltpu.VMEM((documents, 2 * tokens), BF16),
        ],
        out_shape=jax.ShapeDtypeStruct((documents, rows_block * kept), F32),
        name="fold",
        compiler_params=params(16),
        cost_estimate=pl.CostEstimate(flops=32_000_000, bytes_accessed=1 << 20, transcendentals=0),
    )(ids, lengths, spread, order, left, own, *mine, *theirs)


def mix_kernel(blocks, kept, scale, in_ref, out_ref):
    rows, lanes = in_ref.shape
    docs = rows // blocks
    tile = 16 * kept
    count = lanes // tile
    row, col = iota((tile, tile), 0), iota((tile, tile), 1)
    over_rows = jnp.bitwise_and(row % 16, col // kept)
    over_cols = jnp.bitwise_and(row // 16, col % kept)
    table = (parity_sign(over_rows) * parity_sign(over_cols)).astype(BF16)
    stacked = jnp.concatenate([in_ref[:, t * tile:(t + 1) * tile] for t in range(count)], axis=0)
    hi, lo = split_bf16(stacked)
    both = jnp.dot(jnp.concatenate([hi, lo], axis=0), table, preferred_element_type=F32)
    both = both[:count * rows] + both[count * rows:]
    parts = [[both[t * rows + b * docs:t * rows + (b + 1) * docs] for b in range(blocks)] for t in range(count)]

    def butterfly(items):
        step = 1
        while step < len(items):
            for low in range(len(items)):
                if not low & step:
                    a, b = items[low], items[low | step]
                    items[low], items[low | step] = a + b, a - b
            step *= 2
        return items

    for b in range(blocks):
        column = butterfly([parts[t][b] for t in range(count)])
        for t in range(count):
            parts[t][b] = column[t]
    for t in range(count):
        done = butterfly(parts[t])
        for b in range(blocks):
            out_ref[b * docs:(b + 1) * docs, t * tile:(t + 1) * tile] = (done[b] * scale).astype(BF16)


def mix(folded, blocks, kept, scale):
    return pl.pallas_call(
        functools.partial(mix_kernel, blocks, kept, scale),
        in_specs=[VMEM_SPEC],
        out_specs=VMEM_SPEC,
        out_shape=jax.ShapeDtypeStruct(folded.shape, BF16),
        name="mix",
        compiler_params=params(8),
    )(folded)


def project_kernel(ids_ref, kept_ref, other_ref, first_ref, second_ref, out_ref):
    _, width = first_ref.shape
    part = min(512, width)
    for order, (rows_ref, weights_ref) in enumerate(((kept_ref, first_ref), (other_ref, second_ref))):
        layer = ids_ref[0] if order == 0 else 1 - ids_ref[0]

        @pl.loop(0, width // part)
        def _(step):
            col = pl.multiple_of(step * part, part)
            out_ref[:, pl.ds(pl.multiple_of(layer * width + col, 128), part)] = jnp.dot(
                rows_ref[...], weights_ref[:, pl.ds(col, part)], preferred_element_type=F32
            ).astype(out_ref.dtype)


def project(ids, kept, other, first, second):
    documents, depth = kept.shape
    width = first.shape[1]
    return pl.pallas_call(
        project_kernel,
        in_specs=[SMEM_SPEC] + [VMEM_SPEC] * 4,
        out_specs=VMEM_SPEC,
        out_shape=jax.ShapeDtypeStruct((documents, 2 * width), BF16),
        name="project",
        compiler_params=params(8),
        cost_estimate=pl.CostEstimate(
            flops=4 * documents * depth * width, bytes_accessed=4 * depth * width, transcendentals=0
        ),
    )(ids, kept, other, first, second)


def exchange(rows):
    return lax.all_to_all(rows, "blk", split_axis=0, concat_axis=0, tiled=True)


def shards(in_factors, out_factors, lengths, signs, projection):
    blocks = lax.axis_size("blk")
    halves = lax.axis_size("sub")
    my_block = lax.axis_index("blk")
    my_half = lax.axis_index("sub")
    layers, _, tok_local, in_width = in_factors.shape
    out_width = out_factors.shape[3]
    assert layers == halves == 2
    rows_block = in_width // blocks
    documents = lengths.shape[1]
    docs = documents // blocks
    kept_cols = projection.shape[2]
    scale = 1.0 / math.sqrt(in_width * out_width)
    ids = jnp.stack([my_half, my_block]).astype(jnp.int32)
    weights = projection.reshape(layers, rows_block * kept_cols, projection.shape[3])

    routes = [(2 * b, 2 * b + 2) for b in range(blocks - 1)] + [(2 * b + 3, 2 * b + 1) for b in range(blocks - 1)]
    own = out_factors[:, 0]
    mine, theirs = [], []
    for _ in range(1, blocks):
        got = lax.ppermute(mine[-1] if mine else own, ("blk", "sub"), routes)
        mine.append(got)
        theirs.append(lax.ppermute(got, "sub", [(0, 1), (1, 0)]))
    left = lax.dynamic_index_in_dim(in_factors[:, 0], my_half, 0, keepdims=False)
    left = exchange(left.T.reshape(blocks, rows_block, tok_local))
    spread, order = prepare(ids, signs, kept_cols)
    first = fetch(ids, weights, 0)
    second = fetch(ids, weights, 1)
    folded = exchange(fold(ids, lengths, spread, order, left, own, mine, theirs, kept_cols))
    kept = exchange(mix(folded, blocks, kept_cols, scale))
    other = lax.ppermute(kept, "sub", [(0, 1), (1, 0)])
    terms = exchange(project(ids, kept, other, first, second))
    terms = terms.reshape(blocks, docs, layers, weights.shape[2]).astype(F32)
    return jnp.sum(terms, axis=0)[None]


def solution(mesh):
    return jax.shard_map(
        shards,
        mesh=mesh,
        in_specs=(
            P(None, ("parts", "dp"), "blk", None),
            P(None, ("parts", "dp"), "blk", None),
            P(("parts", "dp"), None),
            P(None, "blk", None),
            P(None, "blk", None, "sub"),
        ),
        out_specs=P(("parts", "dp"), "blk", None, "sub"),
        check_vma=False,
    )
```

```python
import functools
import math

import jax
import jax.numpy as jnp
from jax import lax
from jax.experimental import pallas as pl
from jax.experimental.pallas import tpu as pltpu
from jax.sharding import PartitionSpec as P


F32 = jnp.float32
BF16 = jnp.bfloat16
NT = (((1,), (1,)), ((), ()))
FINE = 4
SMEM_SPEC = pl.BlockSpec(memory_space=pltpu.SMEM)
VMEM_SPEC = pl.BlockSpec(memory_space=pltpu.VMEM)
HBM_SPEC = pl.BlockSpec(memory_space=pltpu.HBM)


def params(mib):
    return pltpu.CompilerParams(vmem_limit_bytes=mib << 20)


def iota(shape, dim):
    return lax.broadcasted_iota(jnp.int32, shape, dim)


def parity_sign(values):
    for shift in (8, 4, 2, 1):
        values = jnp.bitwise_xor(values, jnp.right_shift(values, shift))
    return (1 - 2 * jnp.bitwise_and(values, 1)).astype(F32)


def split_bf16(x):
    hi = x.astype(BF16)
    return hi, (x - hi.astype(F32)).astype(BF16)


def prepare_kernel(kept, ids_ref, signs_ref, spread_ref, order_ref):
    _, width = signs_ref.shape[1:]
    coarse = kept // FINE
    part = width // coarse
    source = iota((width, width), 0)
    place = (source // FINE) % coarse * part + source // kept * FINE + source % FINE
    order_ref[...] = jnp.where(place == iota((width, width), 1), 1.0, 0.0).astype(BF16)
    signed = (2 * signs_ref[ids_ref[0]] - 1).astype(F32).astype(BF16)
    for c in range(coarse):
        cols = slice(c * part, (c + 1) * part)
        piece = jnp.dot(signed, order_ref[:, cols], preferred_element_type=F32)
        for f in range(FINE):
            spread_ref[c, f] = jnp.where(iota(piece.shape, 1) % FINE == f, piece, 0.0).astype(BF16)


def prepare(ids, signs, kept):
    rows, width = signs.shape[1:]
    coarse = kept // FINE
    return pl.pallas_call(
        functools.partial(prepare_kernel, kept),
        in_specs=[SMEM_SPEC, VMEM_SPEC],
        out_specs=[VMEM_SPEC, VMEM_SPEC],
        out_shape=[
            jax.ShapeDtypeStruct((coarse, FINE, rows, width // coarse), BF16),
            jax.ShapeDtypeStruct((width, width), BF16),
        ],
        name="prepare",
        compiler_params=params(3),
        cost_estimate=pl.CostEstimate(flops=16_000_000, bytes_accessed=8 * rows * width, transcendentals=0),
    )(ids, signs)


def fetch_kernel(pick, ids_ref, weights_ref, out_ref, sems):
    layer = ids_ref[0] if pick == 0 else 1 - ids_ref[0]
    count = sems.shape[0]
    part = out_ref.shape[0] // count
    copies = [
        pltpu.make_async_copy(
            weights_ref.at[layer, pl.ds(i * part, part)], out_ref.at[pl.ds(i * part, part)], sems.at[i]
        )
        for i in range(count)
    ]
    for copy in copies:
        copy.start()
    for copy in copies:
        copy.wait()


def fetch(ids, weights, pick):
    depth, width = weights.shape[1:]
    return pl.pallas_call(
        functools.partial(fetch_kernel, pick),
        in_specs=[SMEM_SPEC, HBM_SPEC],
        out_specs=VMEM_SPEC,
        out_shape=jax.ShapeDtypeStruct((depth, width), BF16),
        scratch_shapes=[pltpu.SemaphoreType.DMA((4,))],
        name="fetch",
        compiler_params=params(22 if pick == 0 else 16),
        cost_estimate=pl.CostEstimate(flops=16_000_000, bytes_accessed=2 * depth * width, transcendentals=0),
    )(ids, weights)


def fold_kernel(blocks, kept, tile, ids_ref, lengths_ref, spread_ref, order_ref, left_ref, own_ref, *refs):
    mine_refs, theirs_refs = refs[:blocks - 1], refs[blocks - 1:2 * blocks - 2]
    out_ref, b_scr, a_scr, hot_scr = refs[2 * blocks - 2:]
    tokens, width = b_scr.shape
    tok_local = tokens // blocks
    documents = hot_scr.shape[0]
    coarse = kept // FINE
    part = width // coarse
    half, me = ids_ref[0], ids_ref[1]

    @pl.when(pl.program_id(0) == 0)
    def _():
        def place(value, block):
            rows = pl.ds(pl.multiple_of(block * tok_local, tok_local), tok_local)
            b_scr[rows, :] = jnp.dot(value[...], order_ref[...], preferred_element_type=F32).astype(BF16)

        place(own_ref.at[half], me)
        for step in range(1, blocks):
            toward = jnp.where(half == 0, step, -step)
            for value, block in (
                (mine_refs[step - 1].at[half], me - toward),
                (theirs_refs[step - 1].at[half], me + toward),
            ):
                pl.when((block >= 0) & (block < blocks))(functools.partial(place, value, block))
        for block in range(blocks):
            a_scr[:, block * tok_local:(block + 1) * tok_local] = left_ref[block].astype(F32)
        square = (documents, documents)
        spread = jnp.broadcast_to(lengths_ref[...].astype(F32), square)
        ends = jnp.sum(jnp.where(iota(square, 1) <= iota(square, 0), spread, 0.0), axis=1, keepdims=True)
        starts = jnp.sum(jnp.where(iota(square, 1) < iota(square, 0), spread, 0.0), axis=1, keepdims=True)
        token = iota((documents, tokens), 1).astype(F32)
        hot = jnp.where((token >= starts) & (token < ends), 1.0, 0.0).astype(BF16)
        hot_scr[:, :tokens] = hot
        hot_scr[:, tokens:] = hot

    row0 = pl.multiple_of(pl.program_id(0) * tile, tile)
    left = a_scr[pl.ds(row0, tile), :]
    terms = []
    for c in range(coarse):
        signed = spread_ref[c, :, pl.ds(row0, tile), :].reshape(FINE * tile, part)
        mixed = lax.dot_general(signed, b_scr[:, c * part:(c + 1) * part], NT, preferred_element_type=F32)
        mixed = (mixed.reshape(FINE, tile, tokens) * left[None]).reshape(FINE * tile, tokens)
        terms.append(split_bf16(mixed))
    for u in range(tile // 16):
        pieces = [
            jnp.concatenate(
                [terms[c][w][f * tile + u * 16:f * tile + (u + 1) * 16] for c in range(coarse) for f in range(FINE)],
                axis=0,
            )
            for w in range(2)
        ]
        out_ref[:, u * 16 * kept:(u + 1) * 16 * kept] = lax.dot_general(
            hot_scr[...], jnp.concatenate(pieces, axis=1), NT, preferred_element_type=F32
        )


def fold(ids, lengths, spread, order, left, own, mine, theirs, kept):
    blocks, rows_block, tok_local = left.shape
    width = own.shape[2]
    tokens = blocks * tok_local
    documents = lengths.shape[1]
    tile = min(64, rows_block)
    return pl.pallas_call(
        functools.partial(fold_kernel, blocks, kept, tile),
        grid=(rows_block // tile,),
        in_specs=[SMEM_SPEC] + [VMEM_SPEC] * (5 + 2 * (blocks - 1)),
        out_specs=pl.BlockSpec((documents, tile * kept), lambda g: (0, g)),
        scratch_shapes=[
            pltpu.VMEM((tokens, width), BF16),
            pltpu.VMEM((rows_block, tokens), F32),
            pltpu.VMEM((documents, 2 * tokens), BF16),
        ],
        out_shape=jax.ShapeDtypeStruct((documents, rows_block * kept), F32),
        name="fold",
        compiler_params=params(8),
        cost_estimate=pl.CostEstimate(flops=32_000_000, bytes_accessed=1 << 20, transcendentals=0),
    )(ids, lengths, spread, order, left, own, *mine, *theirs)


def mix_kernel(blocks, kept, scale, in_ref, out_ref):
    rows, lanes = in_ref.shape
    docs = rows // blocks
    tile = 16 * kept
    count = lanes // tile
    row, col = iota((tile, tile), 0), iota((tile, tile), 1)
    over_rows = jnp.bitwise_and(row % 16, col // kept)
    over_cols = jnp.bitwise_and(row // 16, col % kept)
    table = (parity_sign(over_rows) * parity_sign(over_cols)).astype(BF16)
    stacked = jnp.concatenate([in_ref[:, t * tile:(t + 1) * tile] for t in range(count)], axis=0)
    hi, lo = split_bf16(stacked)
    both = jnp.dot(jnp.concatenate([hi, lo], axis=0), table, preferred_element_type=F32)
    both = both[:count * rows] + both[count * rows:]
    parts = [[both[t * rows + b * docs:t * rows + (b + 1) * docs] for b in range(blocks)] for t in range(count)]

    def butterfly(items):
        step = 1
        while step < len(items):
            for low in range(len(items)):
                if not low & step:
                    a, b = items[low], items[low | step]
                    items[low], items[low | step] = a + b, a - b
            step *= 2
        return items

    for b in range(blocks):
        column = butterfly([parts[t][b] for t in range(count)])
        for t in range(count):
            parts[t][b] = column[t]
    for t in range(count):
        done = butterfly(parts[t])
        for b in range(blocks):
            out_ref[b * docs:(b + 1) * docs, t * tile:(t + 1) * tile] = (done[b] * scale).astype(BF16)


def mix(folded, blocks, kept, scale):
    return pl.pallas_call(
        functools.partial(mix_kernel, blocks, kept, scale),
        in_specs=[VMEM_SPEC],
        out_specs=VMEM_SPEC,
        out_shape=jax.ShapeDtypeStruct(folded.shape, BF16),
        name="mix",
        compiler_params=params(2),
    )(folded)


def project_kernel(ids_ref, kept_ref, other_ref, first_ref, second_ref, out_ref):
    _, width = first_ref.shape
    part = min(512, width)
    for order, (rows_ref, weights_ref) in enumerate(((kept_ref, first_ref), (other_ref, second_ref))):
        layer = ids_ref[0] if order == 0 else 1 - ids_ref[0]

        @pl.loop(0, width // part)
        def _(step):
            col = pl.multiple_of(step * part, part)
            out_ref[:, pl.ds(pl.multiple_of(layer * width + col, 128), part)] = jnp.dot(
                rows_ref[...], weights_ref[:, pl.ds(col, part)], preferred_element_type=F32
            ).astype(out_ref.dtype)


def project(ids, kept, other, first, second):
    documents, depth = kept.shape
    width = first.shape[1]
    return pl.pallas_call(
        project_kernel,
        in_specs=[SMEM_SPEC] + [VMEM_SPEC] * 4,
        out_specs=VMEM_SPEC,
        out_shape=jax.ShapeDtypeStruct((documents, 2 * width), BF16),
        name="project",
        compiler_params=params(2),
        cost_estimate=pl.CostEstimate(
            flops=4 * documents * depth * width, bytes_accessed=4 * depth * width, transcendentals=0
        ),
    )(ids, kept, other, first, second)


def exchange(rows):
    return lax.all_to_all(rows, "blk", split_axis=0, concat_axis=0, tiled=True)


def shards(in_factors, out_factors, lengths, signs, projection):
    blocks = lax.axis_size("blk")
    halves = lax.axis_size("sub")
    my_block = lax.axis_index("blk")
    my_half = lax.axis_index("sub")
    layers, _, tok_local, in_width = in_factors.shape
    out_width = out_factors.shape[3]
    assert layers == halves == 2
    rows_block = in_width // blocks
    documents = lengths.shape[1]
    docs = documents // blocks
    kept_cols = projection.shape[2]
    scale = 1.0 / math.sqrt(in_width * out_width)
    ids = jnp.stack([my_half, my_block]).astype(jnp.int32)
    weights = projection.reshape(layers, rows_block * kept_cols, projection.shape[3])

    routes = [(2 * b, 2 * b + 2) for b in range(blocks - 1)] + [(2 * b + 3, 2 * b + 1) for b in range(blocks - 1)]
    own = out_factors[:, 0]
    mine, theirs = [], []
    for _ in range(1, blocks):
        got = lax.ppermute(mine[-1] if mine else own, ("blk", "sub"), routes)
        mine.append(got)
        theirs.append(lax.ppermute(got, "sub", [(0, 1), (1, 0)]))
    left = lax.dynamic_index_in_dim(in_factors[:, 0], my_half, 0, keepdims=False)
    left = exchange(left.T.reshape(blocks, rows_block, tok_local))
    spread, order = prepare(ids, signs, kept_cols)
    first = fetch(ids, weights, 0)
    second = fetch(ids, weights, 1)
    folded = exchange(fold(ids, lengths, spread, order, left, own, mine, theirs, kept_cols))
    kept = exchange(mix(folded, blocks, kept_cols, scale))
    other = lax.ppermute(kept, "sub", [(0, 1), (1, 0)])
    terms = exchange(project(ids, kept, other, first, second))
    terms = terms.reshape(blocks, docs, layers, weights.shape[2]).astype(F32)
    return jnp.sum(terms, axis=0)[None]


def solution(mesh):
    return jax.shard_map(
        shards,
        mesh=mesh,
        in_specs=(
            P(None, ("parts", "dp"), "blk", None),
            P(None, ("parts", "dp"), "blk", None),
            P(("parts", "dp"), None),
            P(None, "blk", None),
            P(None, "blk", None, "sub"),
        ),
        out_specs=P(("parts", "dp"), "blk", None, "sub"),
        check_vma=False,
    )
```

```python
import functools
import math

import jax
import jax.numpy as jnp
from jax import lax
from jax.experimental import pallas as pl
from jax.experimental.pallas import tpu as pltpu
from jax.sharding import PartitionSpec as P


F32 = jnp.float32
BF16 = jnp.bfloat16
NT = (((1,), (1,)), ((), ()))
FINE = 4
SMEM_SPEC = pl.BlockSpec(memory_space=pltpu.SMEM)
VMEM_SPEC = pl.BlockSpec(memory_space=pltpu.VMEM)
HBM_SPEC = pl.BlockSpec(memory_space=pltpu.HBM)


def params(mib):
    return pltpu.CompilerParams(vmem_limit_bytes=mib << 20)


def iota(shape, dim):
    return lax.broadcasted_iota(jnp.int32, shape, dim)


def parity_sign(values):
    for shift in (8, 4, 2, 1):
        values = jnp.bitwise_xor(values, jnp.right_shift(values, shift))
    return (1 - 2 * jnp.bitwise_and(values, 1)).astype(F32)


def split_bf16(x):
    hi = x.astype(BF16)
    return hi, (x - hi.astype(F32)).astype(BF16)


def prepare_kernel(kept, ids_ref, signs_ref, spread_ref, order_ref):
    _, width = signs_ref.shape[1:]
    coarse = kept // FINE
    part = width // coarse
    source = iota((width, width), 0)
    place = (source // FINE) % coarse * part + source // kept * FINE + source % FINE
    order_ref[...] = jnp.where(place == iota((width, width), 1), 1.0, 0.0).astype(BF16)
    signed = (2 * signs_ref[ids_ref[0]] - 1).astype(F32).astype(BF16)
    for c in range(coarse):
        cols = slice(c * part, (c + 1) * part)
        piece = jnp.dot(signed, order_ref[:, cols], preferred_element_type=F32)
        for f in range(FINE):
            spread_ref[c, f] = jnp.where(iota(piece.shape, 1) % FINE == f, piece, 0.0).astype(BF16)


def prepare(ids, signs, kept):
    rows, width = signs.shape[1:]
    coarse = kept // FINE
    return pl.pallas_call(
        functools.partial(prepare_kernel, kept),
        in_specs=[SMEM_SPEC, VMEM_SPEC],
        out_specs=[VMEM_SPEC, VMEM_SPEC],
        out_shape=[
            jax.ShapeDtypeStruct((coarse, FINE, rows, width // coarse), BF16),
            jax.ShapeDtypeStruct((width, width), BF16),
        ],
        name="prepare",
        compiler_params=params(3),
        cost_estimate=pl.CostEstimate(flops=16_000_000, bytes_accessed=8 * rows * width, transcendentals=0),
    )(ids, signs)


def fold_kernel(kept, tile, masks, last, *refs):
    ids_ref, lengths_ref, spread_ref, order_ref, left_ref, more_ref, *refs = refs
    right_refs = refs[:len(masks)]
    if last:
        out_ref, b_scr, a_scr, hot_scr = refs[len(masks):]
    else:
        out_ref, first_ref, b_scr, a_scr, hot_scr, sems = refs[len(masks):]
    tokens, width = b_scr.shape
    tok_local = tokens // len(masks)
    documents = hot_scr.shape[0]
    coarse = kept // FINE
    part = width // coarse
    half, me = ids_ref[0], ids_ref[1]

    def copies():
        count = sems.shape[0]
        rows = first_ref.shape[0] // count
        return [
            pltpu.make_async_copy(
                more_ref.at[half, pl.ds(i * rows, rows)], first_ref.at[pl.ds(i * rows, rows)], sems.at[i]
            )
            for i in range(count)
        ]

    @pl.when(pl.program_id(0) == 0)
    def _():
        if not last:
            for copy in copies():
                copy.start()
        for at, (mask, right) in enumerate(zip(masks, right_refs)):
            b_scr[at * tok_local:(at + 1) * tok_local, :] = jnp.dot(
                right[...], order_ref[...], preferred_element_type=F32
            ).astype(BF16)
            a_scr[:, at * tok_local:(at + 1) * tok_local] = left_ref[jnp.bitwise_xor(me, mask)].astype(F32)
        square = (documents, documents)
        spread = jnp.broadcast_to(lengths_ref[...].astype(F32), square)
        ends = jnp.sum(jnp.where(iota(square, 1) <= iota(square, 0), spread, 0.0), axis=1, keepdims=True)
        starts = jnp.sum(jnp.where(iota(square, 1) < iota(square, 0), spread, 0.0), axis=1, keepdims=True)
        place = iota((documents, tokens), 1)
        mask = place // tok_local + masks[0]
        token = (jnp.bitwise_xor(mask, me) * tok_local + place % tok_local).astype(F32)
        hot = jnp.where((token >= starts) & (token < ends), 1.0, 0.0).astype(BF16)
        hot_scr[:, :tokens] = hot
        hot_scr[:, tokens:] = hot

    row0 = pl.multiple_of(pl.program_id(0) * tile, tile)
    left = a_scr[pl.ds(row0, tile), :]
    terms = []
    for c in range(coarse):
        signed = spread_ref[c, :, pl.ds(row0, tile), :].reshape(FINE * tile, part)
        mixed = lax.dot_general(signed, b_scr[:, c * part:(c + 1) * part], NT, preferred_element_type=F32)
        mixed = (mixed.reshape(FINE, tile, tokens) * left[None]).reshape(FINE * tile, tokens)
        terms.append(split_bf16(mixed))
    for u in range(tile // 16):
        pieces = [
            jnp.concatenate(
                [terms[c][w][f * tile + u * 16:f * tile + (u + 1) * 16] for c in range(coarse) for f in range(FINE)],
                axis=0,
            )
            for w in range(2)
        ]
        total = lax.dot_general(
            hot_scr[...], jnp.concatenate(pieces, axis=1), NT, preferred_element_type=F32
        )
        lanes = slice(u * 16 * kept, (u + 1) * 16 * kept)
        out_ref[:, lanes] = total + more_ref[:, lanes] if last else total

    if not last:
        @pl.when(pl.program_id(0) == pl.num_programs(0) - 1)
        def _():
            for copy in copies():
                copy.wait()


def fold(ids, lengths, spread, order, left, rights, masks, kept, weights=None, partial=None):
    _, rows_block, tok_local = left.shape
    width = order.shape[0]
    tokens = len(masks) * tok_local
    documents = lengths.shape[1]
    tile = min(64, rows_block)
    last = weights is None
    out_spec = pl.BlockSpec((documents, tile * kept), lambda g: (0, g))
    out_shape = jax.ShapeDtypeStruct((documents, rows_block * kept), F32)
    scratch = [
        pltpu.VMEM((tokens, width), BF16),
        pltpu.VMEM((rows_block, tokens), F32),
        pltpu.VMEM((documents, 2 * tokens), BF16),
    ]
    return pl.pallas_call(
        functools.partial(fold_kernel, kept, tile, masks, last),
        grid=(rows_block // tile,),
        in_specs=[SMEM_SPEC] + [VMEM_SPEC] * 4 + [out_spec if last else HBM_SPEC] + [VMEM_SPEC] * len(masks),
        out_specs=out_spec if last else [out_spec, VMEM_SPEC],
        scratch_shapes=scratch if last else scratch + [pltpu.SemaphoreType.DMA((4,))],
        out_shape=out_shape if last else [out_shape, jax.ShapeDtypeStruct(weights.shape[1:], BF16)],
        name="last" if last else "early",
        compiler_params=params(8 if last else 20),
        cost_estimate=pl.CostEstimate(flops=32_000_000, bytes_accessed=1 << 20, transcendentals=0),
    )(ids, lengths, spread, order, left, partial if last else weights, *rights)


def mix_kernel(blocks, kept, scale, in_ref, out_ref):
    rows, lanes = in_ref.shape
    docs = rows // blocks
    tile = 16 * kept
    count = lanes // tile
    row, col = iota((tile, tile), 0), iota((tile, tile), 1)
    over_rows = jnp.bitwise_and(row % 16, col // kept)
    over_cols = jnp.bitwise_and(row // 16, col % kept)
    table = (parity_sign(over_rows) * parity_sign(over_cols)).astype(BF16)
    stacked = jnp.concatenate([in_ref[:, t * tile:(t + 1) * tile] for t in range(count)], axis=0)
    hi, lo = split_bf16(stacked)
    both = jnp.dot(jnp.concatenate([hi, lo], axis=0), table, preferred_element_type=F32)
    both = both[:count * rows] + both[count * rows:]
    parts = [[both[t * rows + b * docs:t * rows + (b + 1) * docs] for b in range(blocks)] for t in range(count)]

    def butterfly(items):
        step = 1
        while step < len(items):
            for low in range(len(items)):
                if not low & step:
                    a, b = items[low], items[low | step]
                    items[low], items[low | step] = a + b, a - b
            step *= 2
        return items

    for b in range(blocks):
        column = butterfly([parts[t][b] for t in range(count)])
        for t in range(count):
            parts[t][b] = column[t]
    for t in range(count):
        done = butterfly(parts[t])
        for b in range(blocks):
            out_ref[b * docs:(b + 1) * docs, t * tile:(t + 1) * tile] = (done[b] * scale).astype(BF16)


def mix(folded, blocks, kept, scale):
    return pl.pallas_call(
        functools.partial(mix_kernel, blocks, kept, scale),
        in_specs=[VMEM_SPEC],
        out_specs=VMEM_SPEC,
        out_shape=jax.ShapeDtypeStruct(folded.shape, BF16),
        name="mix",
        compiler_params=params(2),
    )(folded)


def project_kernel(ids_ref, kept_ref, other_ref, first_ref, weights_ref, out_ref, second_ref, sems):
    _, width = first_ref.shape
    count = sems.shape[0]
    part = width // count
    copies = [
        pltpu.make_async_copy(
            weights_ref.at[1 - ids_ref[0], :, pl.ds(i * part, part)], second_ref.at[:, pl.ds(i * part, part)], sems.at[i]
        )
        for i in range(count)
    ]
    for copy in copies:
        copy.start()
    for order, (rows_ref, from_ref) in enumerate(((kept_ref, first_ref), (other_ref, second_ref))):
        layer = ids_ref[0] if order == 0 else 1 - ids_ref[0]
        for i in range(count):
            if order == 1:
                copies[i].wait()
            out_ref[:, pl.ds(pl.multiple_of(layer * width + i * part, 128), part)] = jnp.dot(
                rows_ref[...], from_ref[:, i * part:(i + 1) * part], preferred_element_type=F32
            ).astype(out_ref.dtype)


def project(ids, kept, other, first, weights):
    documents, depth = kept.shape
    width = first.shape[1]
    return pl.pallas_call(
        project_kernel,
        in_specs=[SMEM_SPEC] + [VMEM_SPEC] * 3 + [HBM_SPEC],
        out_specs=VMEM_SPEC,
        out_shape=jax.ShapeDtypeStruct((documents, 2 * width), BF16),
        scratch_shapes=[pltpu.VMEM((depth, width), BF16), pltpu.SemaphoreType.DMA((4,))],
        name="project",
        compiler_params=params(20),
        cost_estimate=pl.CostEstimate(
            flops=4 * documents * depth * width, bytes_accessed=4 * depth * width, transcendentals=0
        ),
    )(ids, kept, other, first, weights)


def exchange(rows):
    return lax.all_to_all(rows, "blk", split_axis=0, concat_axis=0, tiled=True)


def shards(in_factors, out_factors, lengths, signs, projection):
    blocks = lax.axis_size("blk")
    halves = lax.axis_size("sub")
    my_block = lax.axis_index("blk")
    my_half = lax.axis_index("sub")
    layers, _, tok_local, in_width = in_factors.shape
    out_width = out_factors.shape[3]
    assert layers == halves == 2
    rows_block = in_width // blocks
    documents = lengths.shape[1]
    docs = documents // blocks
    kept_cols = projection.shape[2]
    scale = 1.0 / math.sqrt(in_width * out_width)
    ids = jnp.stack([my_half, my_block]).astype(jnp.int32)
    weights = projection.reshape(layers, rows_block * kept_cols, projection.shape[3])

    rights = {0: lax.dynamic_index_in_dim(out_factors[:, 0], my_half, 0, keepdims=False)}
    bit = blocks // 2
    while bit:
        for mask in list(rights):
            rights[mask | bit] = lax.ppermute(rights[mask], "blk", [(b, b ^ bit) for b in range(blocks)])
        bit //= 2
    left = lax.dynamic_index_in_dim(in_factors[:, 0], my_half, 0, keepdims=False)
    left = exchange(left.T.reshape(blocks, rows_block, tok_local))
    spread, order = prepare(ids, signs, kept_cols)
    masks = range(blocks)
    early, late = masks[:-1], masks[-1:]
    partial, first = fold(
        ids, lengths, spread, order, left, [rights[m] for m in early], early, kept_cols, weights=weights
    )
    folded = fold(ids, lengths, spread, order, left, [rights[m] for m in late], late, kept_cols, partial=partial)
    folded = exchange(folded)
    kept = exchange(mix(folded, blocks, kept_cols, scale))
    other = lax.ppermute(kept, "sub", [(0, 1), (1, 0)])
    terms = exchange(project(ids, kept, other, first, weights))
    terms = terms.reshape(blocks, docs, layers, weights.shape[2]).astype(F32)
    return jnp.sum(terms, axis=0)[None]


def solution(mesh):
    return jax.shard_map(
        shards,
        mesh=mesh,
        in_specs=(
            P(None, ("parts", "dp"), "blk", None),
            P(None, ("parts", "dp"), "blk", None),
            P(("parts", "dp"), None),
            P(None, "blk", None),
            P(None, "blk", None, "sub"),
        ),
        out_specs=P(("parts", "dp"), "blk", None, "sub"),
        check_vma=False,
    )
```
